128 devices in a mesh: ga: 16 (over x, z), band: 8 (over y, core).
Axes of the slice: x: 4, y: 4, z: 4, core: 2. Of those that a mesh axis runs over, the one named last changes fastest.
Arguments:
- coeffs: bfloat16 [2, 2048, 40960], P(None, ('ga', 'band')), may hold values from -6 to 6
- projectors: bfloat16 [1280, 2, 40960], P(None, None, 'ga'), may hold values from -0.01953125 to 0.01953125
- block_coupling: float32 [1280, 18], replicated, may hold values from -12 to 12
- atom_counts: int32 [160], replicated, may hold values from 4 to 18, as said below
- wave_counts: int32 [16], P('ga'), may hold values from 1920 to 2560
Outputs:
- applied: bfloat16 [2, 2048, 40960], P(None, ('ga', 'band'))
- band_energy: float32 [2048], P(('ga', 'band'))
- total_energy: float32 [], replicated
The draws below stay inside these ranges and needn't reach their ends.
Inputs may be any that keep to these rules, and one draw needn't show every extreme that they name: `atom_counts`: each atom has 4, 8 or 18 projectors, the counts sum to 1280 and the largest is 18.
All inputs are finite; a program needn't handle non-finite values.
Results may differ from the reference program's by a relative error of at most 0.013.
Values may be sent and summed in bfloat16 or wider, within the bound.
A program may use at most 128 MiB of HBM per device.

```python
import math
import jax
import jax.numpy as jnp
from jax import lax

NG = 40960
ATOMS = 160
MOST = 18
G_DEV = 2560
NB = 2048
NP = 1280
N_GA = 16


def draw_atom_counts(key, part):
    group_pattern = jnp.array([18, 18, 4, 4, 4, 4, 4], jnp.int32)
    heavy_groups = ATOMS // 8
    atom_ids = lax.iota(jnp.int32, ATOMS)
    species = jnp.where(atom_ids < 7 * heavy_groups, group_pattern[atom_ids % 7], 8).astype(jnp.int32)
    return jax.random.permutation(jax.random.fold_in(key, 31), species).astype(jnp.int32)


def with_ends(entries, key, smallest, largest):
    spot = [jax.random.randint(jax.random.fold_in(key, axis), (), 0, length) for axis, length in enumerate(entries.shape)]
    widest = entries.shape.index(max(entries.shape))
    next_to = spot[:widest] + [(spot[widest] + 1) % entries.shape[widest]] + spot[widest + 1:]
    return entries.at[tuple(spot)].set(smallest).at[tuple(next_to)].set(largest)


def level_of(stream_key, extent, cuts, smallest, largest):
    loudness = 1.0
    for axis_at, shards_of in cuts:
        steps = jax.random.uniform(jax.random.fold_in(jax.random.fold_in(stream_key, 6), axis_at), (shards_of,), jnp.float32, smallest / len(cuts), largest / len(cuts))
        loudness = loudness * jnp.repeat(jnp.exp(steps), extent[axis_at] // shards_of).reshape((-1,) + (1,) * (len(extent) - 1 - axis_at))
    return loudness


def noise(own_key, extent, spread, most, pieces=(), kind=jnp.bfloat16):
    gain = level_of(own_key, extent, pieces, -0.22, 0.18) if pieces else 1.0
    values = jax.random.normal(own_key, extent, jnp.float32) * spread * gain
    return jnp.minimum(jnp.maximum(values, -most), most).astype(kind)


def setup_inputs(seed: int = 0) -> dict:
    streams_of = jax.random.split(jax.random.key(seed), 6)
    return {
        "coeffs": noise(streams_of[0], (2, NB, NG), 1.0, 6.0, ((1, 128),)),
        "projectors": noise(streams_of[1], (NP, 2, NG), (2 * NG) ** -0.5, 0.01953125, ((2, 16),)),
        "block_coupling": noise(streams_of[2], (NP, MOST), 2.0, 12.0, (), jnp.float32),
        "atom_counts": draw_atom_counts(jax.random.fold_in(streams_of[5], 71), 0),
        "wave_counts": with_ends(jax.random.randint(streams_of[4], (N_GA,), G_DEV * 3 // 4, G_DEV + 1), jax.random.fold_in(streams_of[4], 1), G_DEV * 3 // 4, G_DEV).astype(jnp.int32),
    }


def block_tables(atom_counts, row_ids):
    atom_ends = jnp.cumsum(atom_counts).astype(jnp.int32)
    atom_starts = (atom_ends - atom_counts).astype(jnp.int32)
    inside = (atom_starts[None, :] <= row_ids[:, None]) & (atom_ends[None, :] > row_ids[:, None])
    block_first = lax.optimization_barrier(jnp.sum(jnp.where(inside, atom_starts[None, :], 0), axis=1)).astype(jnp.int32)
    block_length = lax.optimization_barrier(jnp.sum(jnp.where(inside, atom_counts[None, :], 0), axis=1)).astype(jnp.int32)
    return (block_first, block_length)

def couple_rows(values, block_first, block_length, coupling_rows, row_base):
    last_row = values.shape[0] - 1
    summed = jnp.zeros((coupling_rows.shape[0], values.shape[1]), jnp.float32)
    for offset in range(coupling_rows.shape[1]):
        source = jnp.clip(block_first + offset - row_base, 0, last_row).astype(jnp.int32)
        column = coupling_rows[:, offset]
        weight = jnp.where(offset < block_length, column, jnp.zeros_like(column))
        summed = summed + weight[:, None] * jnp.take(values, source, axis=0)
    return summed

def reference(coeffs, projectors, block_coupling, atom_counts, wave_counts):
    slot_ids = lax.iota(jnp.int32, NG)
    in_sphere = (slot_ids % G_DEV < wave_counts[slot_ids // G_DEV]).astype(jnp.float32)
    masked = coeffs * in_sphere.astype(coeffs.dtype)
    real_part = masked[0]
    imag_part = masked[1]
    stacked = jnp.concatenate([jnp.concatenate([real_part, imag_part], 1), jnp.concatenate([imag_part, -real_part], 1)], 0)
    flat_beta = projectors.reshape(NP, 2 * NG)
    projections = lax.dot_general(flat_beta, stacked, (((1,), (1,)), ((), ())), preferred_element_type=jnp.float32)
    block_first, block_length = block_tables(atom_counts, lax.iota(jnp.int32, NP))
    coupled = couple_rows(projections, block_first, block_length, block_coupling, 0)
    energy_terms = lax.optimization_barrier(jnp.sum(projections * coupled, axis=0))
    band_energy = (energy_terms[:NB] + energy_terms[NB:]) / NP
    total_energy = jnp.sum(band_energy) / math.sqrt(NB)
    products = lax.dot_general(coupled.astype(jnp.bfloat16), flat_beta, (((0,), (0,)), ((), ())), preferred_element_type=jnp.float32)
    real_out = products[:NB, :NG] - products[NB:, NG:]
    imag_out = products[:NB, NG:] + products[NB:, :NG]
    applied = (jnp.stack([real_out, imag_out]) * in_sphere).astype(jnp.bfloat16)
    return (applied, band_energy, total_energy)
```

```python
import math

import jax
import jax.numpy as jnp
from jax import lax
from jax.experimental import pallas as pl
from jax.experimental.pallas import tpu as pltpu
from jax.sharding import PartitionSpec as P

MESH = pl.DeviceIdType.MESH
SIDE = 4
GROUP = 4
REACH = 17

PLACES = [(0, 0)] + sorted(
    [(dx, dz) for dx in range(SIDE) for dz in range(SIDE) if (dx, dz) != (0, 0)],
    key=lambda o: min(o[0], SIDE - o[0]) + min(o[1], SIDE - o[1]),
)


def kernel(
    counts_ref,
    waves_ref,
    coupling_ref,
    coeffs_ref,
    proj_ref,
    out_ref,
    energy_ref,
    total_ref,
    beta,
    moved,
    lhs,
    part,
    parts_in,
    mixed,
    mixed_in,
    prod,
    weights,
    mask,
    own_energy,
    energy_in,
    group_energy,
    band_in,
    beta_sem,
    own_sem,
    in_sems,
    part_sems,
    mixed_sems,
    out_sems,
    energy_sems,
    band_sems,
):
    n_ga = len(PLACES)
    n_band = lax.axis_size("band")
    own = mixed.shape[0]
    slots = moved.shape[2]
    rows = beta.shape[0]
    tile = 256
    ga = lax.axis_index("ga")
    band = lax.axis_index("band")
    gx, gz = ga // SIDE, ga % SIDE

    def ahead(n):
        dx, dz = PLACES[n]
        return lax.rem(gx + dx, SIDE) * SIDE + lax.rem(gz + dz, SIDE)

    def behind(n):
        dx, dz = PLACES[n]
        return lax.rem(gx + SIDE - dx, SIDE) * SIDE + lax.rem(gz + SIDE - dz, SIDE)

    def columns(index):
        return pl.ds(pl.multiple_of(index * slots, 128), slots)

    def send(src, dst, sems, n, target):
        return pltpu.make_async_remote_copy(
            src, dst, sems.at[0, n], sems.at[1, n], device_id=target, device_id_type=MESH
        )

    beta_copy = pltpu.make_async_copy(proj_ref.reshape(rows, slots), beta, beta_sem)
    own_copy = pltpu.make_async_copy(coeffs_ref.at[:, columns(ga)], moved.at[0], own_sem.at[0])
    own_copy.start()

    barrier = pltpu.get_barrier_semaphore()
    for n in range(1, n_ga):
        pl.semaphore_signal(barrier, inc=1, device_id={"ga": ahead(n)}, device_id_type=MESH)
    for n in range(1, n_band):
        target = {"band": lax.rem(band + n, n_band)}
        pl.semaphore_signal(barrier, inc=1, device_id=target, device_id_type=MESH)
    pl.semaphore_wait(barrier, n_ga + n_band - 2)

    in_copies = [None]
    for n in range(1, n_ga):
        peer = ahead(n)
        in_copies.append(
            send(coeffs_ref.at[:, columns(peer)], moved.at[n], in_sems, n, {"ga": peer})
        )
        in_copies[n].start()
    beta_copy.start()

    slot_ids = lax.broadcasted_iota(jnp.int32, mask.shape, 1)
    mask[...] = jnp.where(slot_ids < waves_ref[0], 1.0, 0.0)
    atoms = counts_ref.shape[1]
    counts = jnp.broadcast_to(counts_ref[...], (atoms, atoms))
    lane_ids = lax.broadcasted_iota(jnp.int32, (atoms, atoms), 1)
    row_ids = lax.broadcasted_iota(jnp.int32, (atoms, atoms), 0)
    starts = jnp.sum(jnp.where(lane_ids < row_ids, counts, 0.0), axis=1, keepdims=True)
    lengths = jnp.sum(jnp.where(lane_ids == row_ids, counts, 0.0), axis=1, keepdims=True)
    most = coupling_ref.shape[0]
    half = tile // 2
    spread = jnp.where(
        lax.broadcasted_iota(jnp.int32, (half, tile), 1) // 2
        == lax.broadcasted_iota(jnp.int32, (half, tile), 0),
        1.0,
        0.0,
    )

    def weights_of(t, carry):
        at = pl.ds(pl.multiple_of(t * tile, tile), tile)
        halved = coupling_ref[:, pl.ds(pl.multiple_of(t * half, half), half)]
        pairs = jnp.dot(
            halved, spread, precision=lax.Precision.HIGHEST, preferred_element_type=jnp.float32
        )
        ids = t * half + lax.broadcasted_iota(jnp.int32, (atoms, tile), 1) // 2
        ids = ids.astype(jnp.float32)
        inside = (starts <= ids) & (ids < starts + lengths)
        first = jnp.sum(jnp.where(inside, starts, 0.0), axis=0, keepdims=True)
        length = jnp.sum(jnp.where(inside, lengths, 0.0), axis=0, keepdims=True)
        shape = (weights.shape[0], tile)
        shift = lax.broadcasted_iota(jnp.int32, shape, 0).astype(jnp.float32) - REACH
        place = shift + (ids[0:1] - first)
        sums = jnp.zeros(shape, jnp.float32)
        for k in range(most):
            row = jnp.where(k < length, pairs[k : k + 1], 0.0)
            sums = sums + jnp.where(place == k, row, 0.0)
        weights[:, at] = sums
        return carry

    lax.fori_loop(0, rows // tile, weights_of, 0)

    def even_lanes(shape):
        return lax.broadcasted_iota(jnp.int32, shape, len(shape) - 1) % 2 == 0

    def swapped(values, even):
        last = values.shape[-1]
        dim = len(values.shape) - 1
        return jnp.where(even, pltpu.roll(values, last - 1, dim), pltpu.roll(values, 1, dim))

    beta_copy.wait()
    part_copies = [None] * n_ga
    for first in range(0, n_ga, GROUP):
        for n in range(first, first + GROUP):
            if n == 0:
                own_copy.wait()
            else:
                in_copies[n].wait_recv()
        seen = mask[0:1, :].astype(jnp.bfloat16)
        lhs[...] = moved[first : first + GROUP].reshape(lhs.shape) * seen

        def project(t, carry):
            at = pl.ds(pl.multiple_of(t * tile, tile), tile)
            sums = lax.dot_general(
                lhs[...],
                beta[at, :],
                (((1,), (1,)), ((), ())),
                preferred_element_type=jnp.float32,
            )
            even = even_lanes((own, tile))
            for k in range(GROUP):
                real = sums[2 * own * k : 2 * own * k + own]
                imag = sums[2 * own * k + own : 2 * own * (k + 1)]
                pairs = jnp.where(even, real, -real) + swapped(imag, even)
                part[first + k, :, at] = pairs.astype(jnp.bfloat16)
            return carry

        lax.fori_loop(0, rows // tile, project, 0)
        for n in range(max(first, 1), first + GROUP):
            part_copies[n] = send(part.at[n], parts_in.at[n], part_sems, n, {"ga": behind(n)})
            part_copies[n].start()

    summed = part[0].astype(jnp.float32)
    for n in range(1, n_ga):
        part_copies[n].wait_recv()
        summed = summed + parts_in[n].astype(jnp.float32)
    coupled = jnp.zeros_like(summed)
    for d in range(-REACH, REACH + 1):
        moved_by = pltpu.roll(summed, (-2 * d) % rows, 1) if d else summed
        coupled = coupled + weights[d + REACH : d + REACH + 1, :] * moved_by
    mixed[...] = coupled.astype(jnp.bfloat16)
    mixed_in[0] = mixed[...]
    mixed_copies = [None]
    for n in range(1, n_ga):
        mixed_copies.append(send(mixed, mixed_in.at[n], mixed_sems, n, {"ga": ahead(n)}))
        mixed_copies[n].start()
    terms = jnp.sum(summed * coupled, axis=1, keepdims=True) / (rows // 2)
    diagonal = lax.broadcasted_iota(jnp.int32, (own, 128), 0) == lax.broadcasted_iota(
        jnp.int32, (own, 128), 1
    )
    terms_row = jnp.sum(jnp.where(diagonal, terms, 0.0), axis=0, keepdims=True)
    energy_ref[...] = terms_row
    own_energy[...] = jnp.broadcast_to(jnp.sum(terms, axis=0, keepdims=True), own_energy.shape)
    energy_copies = []
    for n in range(1, n_ga):
        energy_copies.append(
            send(own_energy, energy_in.at[ga], energy_sems, n, {"ga": ahead(n)})
        )
        energy_copies[-1].start()

    out_copies = [None] * n_ga
    for first in range(0, n_ga, GROUP):
        for n in range(max(first, 1), first + GROUP):
            mixed_copies[n].wait_recv()
        even = even_lanes((own, rows))
        for k in range(GROUP):
            values = mixed_in[first + k].astype(jnp.float32)
            lhs[2 * own * k : 2 * own * k + own, :] = jnp.where(even, values, -values).astype(
                jnp.bfloat16
            )
            lhs[2 * own * k + own : 2 * own * (k + 1), :] = swapped(values, even).astype(
                jnp.bfloat16
            )

        def apply(t, carry):
            at = pl.ds(pl.multiple_of(t * tile, tile), tile)
            sums = jnp.dot(lhs[...], beta[:, at], preferred_element_type=jnp.float32)
            sums = sums * mask[0:1, at]
            prod[first : first + GROUP, :, at] = sums.astype(jnp.bfloat16).reshape(
                GROUP, 2 * own, tile
            )
            return carry

        lax.fori_loop(0, slots // tile, apply, 0)
        for n in range(first, first + GROUP):
            place = out_ref.at[:, columns(ga)]
            if n == 0:
                out_copies[0] = pltpu.make_async_copy(prod.at[0], place, own_sem.at[1])
            else:
                out_copies[n] = send(prod.at[n], place, out_sems, n, {"ga": behind(n)})
            out_copies[n].start()

    for copy in energy_copies:
        copy.wait_recv()
    energy_in[pl.ds(ga, 1)] = own_energy[...][None]
    sums = energy_in[0]
    for n in range(1, n_ga):
        sums = sums + energy_in[n]
    group_energy[...] = sums
    band_copies = []
    for n in range(1, n_band):
        target = {"band": lax.rem(band + n, n_band)}
        band_copies.append(send(group_energy, band_in.at[band], band_sems, n, target))
        band_copies[-1].start()
    for copy in band_copies:
        copy.wait_recv()
    band_in[pl.ds(band, 1)] = sums[None]
    sums = band_in[0]
    for n in range(1, n_band):
        sums = sums + band_in[n]
    total_ref[...] = sums / math.sqrt(own * n_ga * n_band)

    for n in range(n_ga):
        if n == 0:
            out_copies[0].wait()
        else:
            out_copies[n].wait_recv()
    for n in range(1, n_ga):
        in_copies[n].wait_send()
        part_copies[n].wait_send()
        mixed_copies[n].wait_send()
        energy_copies[n - 1].wait_send()
        out_copies[n].wait_send()
    for copy in band_copies:
        copy.wait_send()


def shards(coeffs, projectors, block_coupling, atom_counts, wave_counts):
    parts, own, slots_all = coeffs.shape
    rows = projectors.shape[0] * parts
    slots = projectors.shape[2]
    n_ga = lax.axis_size("ga")
    n_band = lax.axis_size("band")
    low, full = jnp.bfloat16, jnp.float32
    vmem = pl.BlockSpec(memory_space=pltpu.VMEM)
    anywhere = pl.BlockSpec(memory_space=pl.ANY)
    applied, energy, total = pl.pallas_call(
        kernel,
        out_shape=[
            jax.ShapeDtypeStruct((parts * own, slots_all), low),
            jax.ShapeDtypeStruct((1, 128), full),
            jax.ShapeDtypeStruct((8, 128), full),
        ],
        in_specs=[vmem, pl.BlockSpec(memory_space=pltpu.SMEM), vmem, anywhere, anywhere],
        out_specs=[anywhere, vmem, vmem],
        scratch_shapes=[
            pltpu.VMEM((rows, slots), low),
            pltpu.VMEM((n_ga, parts * own, slots), low),
            pltpu.VMEM((GROUP * parts * own, slots), low),
            pltpu.VMEM((n_ga, own, rows), low),
            pltpu.VMEM((n_ga, own, rows), low),
            pltpu.VMEM((own, rows), low),
            pltpu.VMEM((n_ga, own, rows), low),
            pltpu.VMEM((n_ga, parts * own, slots), low),
            pltpu.VMEM((40, rows), full),
            pltpu.VMEM((8, slots), full),
            pltpu.VMEM((8, 128), full),
            pltpu.VMEM((n_ga, 8, 128), full),
            pltpu.VMEM((8, 128), full),
            pltpu.VMEM((n_band, 8, 128), full),
            pltpu.SemaphoreType.DMA,
            pltpu.SemaphoreType.DMA((2,)),
            pltpu.SemaphoreType.DMA((2, n_ga)),
            pltpu.SemaphoreType.DMA((2, n_ga)),
            pltpu.SemaphoreType.DMA((2, n_ga)),
            pltpu.SemaphoreType.DMA((2, n_ga)),
            pltpu.SemaphoreType.DMA((2, n_ga)),
            pltpu.SemaphoreType.DMA((2, n_band)),
        ],
        compiler_params=pltpu.CompilerParams(
            collective_id=0, has_side_effects=True, vmem_limit_bytes=56 << 20
        ),
    )(
        atom_counts.astype(full).reshape(1, -1),
        wave_counts,
        block_coupling.T,
        coeffs.reshape(parts * own, slots_all),
        projectors,
    )
    return applied.reshape(coeffs.shape), energy[0, :own], total[0, 0]


def solution(mesh):
    return jax.shard_map(
        shards,
        mesh=mesh,
        in_specs=(P(None, ("ga", "band"), None), P(None, None, "ga"), P(), P(), P("ga")),
        out_specs=(P(None, ("ga", "band"), None), P(("ga", "band")), P()),
        check_vma=False,
    )
```

```python
import math

import jax
import jax.numpy as jnp
from jax import lax
from jax.experimental import pallas as pl
from jax.experimental.pallas import tpu as pltpu
from jax.sharding import PartitionSpec as P

MESH = pl.DeviceIdType.MESH
SIDE = 4
REACH = 17

PLACES = [(0, 0)] + sorted(
    [(dx, dz) for dx in range(SIDE) for dz in range(SIDE) if (dx, dz) != (0, 0)],
    key=lambda o: min(o[0], SIDE - o[0]) + min(o[1], SIDE - o[1]),
)


def kernel(
    counts_ref,
    waves_ref,
    coupling_ref,
    coeffs_ref,
    proj_ref,
    out_ref,
    energy_ref,
    total_ref,
    beta,
    moved,
    lhs,
    part,
    parts_in,
    mixed,
    mixed_in,
    prod,
    weights,
    mask,
    own_energy,
    energy_in,
    group_energy,
    band_in,
    beta_sem,
    own_sem,
    in_sems,
    part_sems,
    mixed_sems,
    out_sems,
    energy_sems,
    band_sems,
):
    n_ga = len(PLACES)
    n_band = lax.axis_size("band")
    half = mixed.shape[1]
    own = 2 * half
    slots = moved.shape[3]
    rows = beta.shape[0]
    tile = 256
    ga = lax.axis_index("ga")
    band = lax.axis_index("band")
    gx, gz = ga // SIDE, ga % SIDE

    def ahead(n):
        dx, dz = PLACES[n]
        return lax.rem(gx + dx, SIDE) * SIDE + lax.rem(gz + dz, SIDE)

    def behind(n):
        dx, dz = PLACES[n]
        return lax.rem(gx + SIDE - dx, SIDE) * SIDE + lax.rem(gz + SIDE - dz, SIDE)

    def columns(index):
        return pl.ds(pl.multiple_of(index * slots, 128), slots)

    def send(src, dst, sems, at, target):
        return pltpu.make_async_remote_copy(
            src,
            dst,
            sems.at[(0, *at)],
            sems.at[(1, *at)],
            device_id=target,
            device_id_type=MESH,
        )

    flat_proj = proj_ref.reshape(rows, slots)
    beta_copy = pltpu.make_async_copy(flat_proj, beta, beta_sem)

    def load_beta(t, carry):
        at = pl.ds(pl.multiple_of(t * tile, tile), tile)
        pltpu.make_async_copy(flat_proj.at[at], beta.at[at], beta_sem).start()
        return carry

    lax.fori_loop(0, rows // tile, load_beta, 0)

    def bands(h, c):
        return pl.ds(c * own + h * half, half)

    def part_rows(c):
        return pl.ds(c * half, half)

    own_copies = []
    for h in range(2):
        for c in range(2):
            own_copies.append(
                pltpu.make_async_copy(
                    coeffs_ref.at[bands(h, c), columns(ga)],
                    moved.at[h, 0, part_rows(c)],
                    own_sem.at[h, c],
                )
            )
            own_copies[-1].start()

    barrier = pltpu.get_barrier_semaphore()
    for n in range(1, n_ga):
        pl.semaphore_signal(barrier, inc=1, device_id={"ga": ahead(n)}, device_id_type=MESH)
    for n in range(1, n_band):
        target = {"band": lax.rem(band + n, n_band)}
        pl.semaphore_signal(barrier, inc=1, device_id=target, device_id_type=MESH)
    pl.semaphore_wait(barrier, n_ga + n_band - 2)

    in_copies = [[], []]
    for h in range(2):
        for n in range(1, n_ga):
            peer = ahead(n)
            for c in range(2):
                copy = send(
                    coeffs_ref.at[bands(h, c), columns(peer)],
                    moved.at[h, n, part_rows(c)],
                    in_sems,
                    (h, n, c),
                    {"ga": peer},
                )
                copy.start()
                in_copies[h].append(copy)

    slot_ids = lax.broadcasted_iota(jnp.int32, mask.shape, 1)
    mask[...] = jnp.where(slot_ids < waves_ref[0], 1.0, 0.0)
    atoms = counts_ref.shape[1]
    counts = jnp.broadcast_to(counts_ref[...].astype(jnp.float32), (atoms, atoms))
    lane_ids = lax.broadcasted_iota(jnp.int32, (atoms, atoms), 1)
    row_ids = lax.broadcasted_iota(jnp.int32, (atoms, atoms), 0)
    starts = jnp.sum(jnp.where(lane_ids < row_ids, counts, 0.0), axis=1, keepdims=True)
    lengths = jnp.sum(jnp.where(lane_ids == row_ids, counts, 0.0), axis=1, keepdims=True)
    most = coupling_ref.shape[0]
    narrow = tile // 2
    spread = jnp.where(
        lax.broadcasted_iota(jnp.int32, (narrow, tile), 1) // 2
        == lax.broadcasted_iota(jnp.int32, (narrow, tile), 0),
        1.0,
        0.0,
    )

    def weights_of(t, carry):
        at = pl.ds(pl.multiple_of(t * tile, tile), tile)
        halved = coupling_ref[:, pl.ds(pl.multiple_of(t * narrow, narrow), narrow)]
        pairs = jnp.dot(
            halved, spread, precision=lax.Precision.HIGHEST, preferred_element_type=jnp.float32
        )
        ids = t * narrow + lax.broadcasted_iota(jnp.int32, (atoms, tile), 1) // 2
        ids = ids.astype(jnp.float32)
        inside = (starts <= ids) & (ids < starts + lengths)
        first = jnp.sum(jnp.where(inside, starts, 0.0), axis=0, keepdims=True)
        length = jnp.sum(jnp.where(inside, lengths, 0.0), axis=0, keepdims=True)
        shape = (weights.shape[0], tile)
        shift = lax.broadcasted_iota(jnp.int32, shape, 0).astype(jnp.float32) - REACH
        place = shift + (ids[0:1] - first)
        sums = jnp.zeros(shape, jnp.float32)
        for k in range(most):
            row = jnp.where(k < length, pairs[k : k + 1], 0.0)
            sums = sums + jnp.where(place == k, row, 0.0)
        weights[:, at] = sums
        return carry

    lax.fori_loop(0, rows // tile, weights_of, 0)

    def even_lanes(shape):
        return lax.broadcasted_iota(jnp.int32, shape, len(shape) - 1) % 2 == 0

    def swapped(values, even):
        last = values.shape[-1]
        dim = len(values.shape) - 1
        return jnp.where(even, pltpu.roll(values, last - 1, dim), pltpu.roll(values, 1, dim))

    def project_half(h):
        for copy in own_copies[2 * h : 2 * h + 2]:
            copy.wait()
        for copy in in_copies[h]:
            copy.wait_recv()
        seen = mask[0:1, :].astype(jnp.bfloat16)
        lhs[...] = moved[h].reshape(lhs.shape) * seen

        def project(t, carry):
            at = pl.ds(pl.multiple_of(t * tile, tile), tile)
            sums = lax.dot_general(
                lhs[...],
                beta[at, :],
                (((1,), (1,)), ((), ())),
                preferred_element_type=jnp.float32,
            ).reshape(n_ga, 2, half, tile)
            even = even_lanes((n_ga, half, tile))
            real, imag = sums[:, 0], sums[:, 1]
            pairs = jnp.where(even, real, -real) + swapped(imag, even)
            part[h, :, :, at] = pairs.astype(jnp.bfloat16)
            return carry

        lax.fori_loop(0, rows // tile, project, 0)
        copies = [None]
        for n in range(1, n_ga):
            copies.append(
                send(part.at[h, n], parts_in.at[h, n], part_sems, (h, n), {"ga": behind(n)})
            )
            copies[n].start()
        return copies

    def couple_half(h, part_copies):
        summed = part[h, 0].astype(jnp.float32)
        for n in range(1, n_ga):
            part_copies[n].wait_recv()
            summed = summed + parts_in[h, n].astype(jnp.float32)
        coupled = jnp.zeros_like(summed)
        for d in range(-REACH, REACH + 1):
            moved_by = pltpu.roll(summed, (-2 * d) % rows, 1) if d else summed
            coupled = coupled + weights[d + REACH : d + REACH + 1, :] * moved_by
        mixed[h] = coupled.astype(jnp.bfloat16)
        mixed_in[h, 0] = mixed[h]
        copies = [None]
        for n in range(1, n_ga):
            copies.append(
                send(mixed.at[h], mixed_in.at[h, n], mixed_sems, (h, n), {"ga": ahead(n)})
            )
            copies[n].start()
        terms = jnp.sum(summed * coupled, axis=1, keepdims=True) / (rows // 2)
        diagonal = lax.broadcasted_iota(
            jnp.int32, (half, 128), 0
        ) + h * half == lax.broadcasted_iota(jnp.int32, (half, 128), 1)
        return copies, jnp.sum(jnp.where(diagonal, terms, 0.0), axis=0, keepdims=True)

    def apply_half(h, mixed_copies):
        for n in range(1, n_ga):
            mixed_copies[n].wait_recv()

        def operand(n, carry):
            values = mixed_in[h, n].astype(jnp.float32)
            even = even_lanes(values.shape)
            both = jnp.concatenate(
                [jnp.where(even, values, -values), swapped(values, even)], axis=0
            )
            lhs[pl.ds(pl.multiple_of(n * own, own), own), :] = both.astype(jnp.bfloat16)
            return carry

        lax.fori_loop(0, n_ga, operand, 0)

        def apply(t, carry):
            at = pl.ds(pl.multiple_of(t * tile, tile), tile)
            sums = jnp.dot(lhs[...], beta[:, at], preferred_element_type=jnp.float32)
            sums = sums * mask[0:1, at]
            prod[h, :, :, at] = sums.astype(jnp.bfloat16).reshape(n_ga, own, tile)
            return carry

        lax.fori_loop(0, slots // tile, apply, 0)
        copies = []
        for n in range(1, n_ga):
            for c in range(2):
                copies.append(
                    send(
                        prod.at[h, n, part_rows(c)],
                        out_ref.at[bands(h, c), columns(ga)],
                        out_sems,
                        (h, n, c),
                        {"ga": behind(n)},
                    )
                )
                copies[-1].start()
        kept = []
        for c in range(2):
            kept.append(
                pltpu.make_async_copy(
                    prod.at[h, 0, part_rows(c)],
                    out_ref.at[bands(h, c), columns(ga)],
                    own_sem.at[2 + h, c],
                )
            )
            kept[-1].start()
        return copies, kept

    beta_copy.wait()
    first_parts = project_half(0)
    second_parts = project_half(1)
    first_mixed, first_terms = couple_half(0, first_parts)
    second_mixed, second_terms = couple_half(1, second_parts)
    terms = first_terms + second_terms
    energy_ref[...] = terms[0, :own]
    own_energy[...] = jnp.broadcast_to(jnp.sum(terms, axis=1, keepdims=True), own_energy.shape)
    energy_copies = []
    for n in range(1, n_ga):
        energy_copies.append(
            send(own_energy, energy_in.at[ga], energy_sems, (n,), {"ga": ahead(n)})
        )
        energy_copies[-1].start()
    first_out, first_kept = apply_half(0, first_mixed)
    second_out, second_kept = apply_half(1, second_mixed)

    for copy in energy_copies:
        copy.wait_recv()
    energy_in[pl.ds(ga, 1)] = own_energy[...][None]
    sums = energy_in[0]
    for n in range(1, n_ga):
        sums = sums + energy_in[n]
    group_energy[...] = sums
    band_copies = []
    for n in range(1, n_band):
        target = {"band": lax.rem(band + n, n_band)}
        band_copies.append(send(group_energy, band_in.at[band], band_sems, (n,), target))
        band_copies[-1].start()
    for copy in band_copies:
        copy.wait_recv()
    band_in[pl.ds(band, 1)] = sums[None]
    sums = band_in[0]
    for n in range(1, n_band):
        sums = sums + band_in[n]
    total_ref[...] = sums[0:1, 0:1] / math.sqrt(own * n_ga * n_band)

    for copy in first_kept + second_kept:
        copy.wait()
    for copy in first_out + second_out:
        copy.wait_recv()
    sent = first_parts[1:] + second_parts[1:] + first_mixed[1:] + second_mixed[1:]
    for copy in in_copies[0] + in_copies[1] + sent + first_out + second_out:
        copy.wait_send()
    for copy in energy_copies + band_copies:
        copy.wait_send()


def shards(coeffs, projectors, block_coupling, atom_counts, wave_counts):
    parts, own, slots_all = coeffs.shape
    rows = projectors.shape[0] * parts
    slots = projectors.shape[2]
    n_ga = lax.axis_size("ga")
    n_band = lax.axis_size("band")
    low, full = jnp.bfloat16, jnp.float32
    vmem = pl.BlockSpec(memory_space=pltpu.VMEM)
    anywhere = pl.BlockSpec(memory_space=pl.ANY)
    applied, energy, total = pl.pallas_call(
        kernel,
        out_shape=[
            jax.ShapeDtypeStruct((parts * own, slots_all), low),
            jax.ShapeDtypeStruct((own,), full),
            jax.ShapeDtypeStruct((1, 1), full),
        ],
        in_specs=[vmem, pl.BlockSpec(memory_space=pltpu.SMEM), vmem, anywhere, anywhere],
        out_specs=[anywhere, vmem, vmem],
        scratch_shapes=[
            pltpu.VMEM((rows, slots), low),
            pltpu.VMEM((2, n_ga, own, slots), low),
            pltpu.VMEM((n_ga * own, slots), low),
            pltpu.VMEM((2, n_ga, own // 2, rows), low),
            pltpu.VMEM((2, n_ga, own // 2, rows), low),
            pltpu.VMEM((2, own // 2, rows), low),
            pltpu.VMEM((2, n_ga, own // 2, rows), low),
            pltpu.VMEM((2, n_ga, own, slots), low),
            pltpu.VMEM((40, rows), full),
            pltpu.VMEM((8, slots), full),
            pltpu.VMEM((8, 128), full),
            pltpu.VMEM((n_ga, 8, 128), full),
            pltpu.VMEM((8, 128), full),
            pltpu.VMEM((n_band, 8, 128), full),
            pltpu.SemaphoreType.DMA,
            pltpu.SemaphoreType.DMA((4, 2)),
            pltpu.SemaphoreType.DMA((2, 2, n_ga, 2)),
            pltpu.SemaphoreType.DMA((2, 2, n_ga)),
            pltpu.SemaphoreType.DMA((2, 2, n_ga)),
            pltpu.SemaphoreType.DMA((2, 2, n_ga, 2)),
            pltpu.SemaphoreType.DMA((2, n_ga)),
            pltpu.SemaphoreType.DMA((2, n_band)),
        ],
        compiler_params=pltpu.CompilerParams(
            collective_id=0, has_side_effects=True, vmem_limit_bytes=56 << 20
        ),
    )(
        atom_counts.reshape(1, -1),
        wave_counts,
        block_coupling.T,
        coeffs.reshape(parts * own, slots_all),
        projectors,
    )
    return applied.reshape(coeffs.shape), energy, total[0, 0]


def solution(mesh):
    return jax.shard_map(
        shards,
        mesh=mesh,
        in_specs=(P(None, ("ga", "band"), None), P(None, None, "ga"), P(), P(), P("ga")),
        out_specs=(P(None, ("ga", "band"), None), P(("ga", "band")), P()),
        check_vma=False,
    )
```

```python
import math

import jax
import jax.numpy as jnp
from jax import lax
from jax.experimental import pallas as pl
from jax.experimental.pallas import tpu as pltpu
from jax.sharding import PartitionSpec as P

MESH = pl.DeviceIdType.MESH
SIDE = 4
REACH = 17

PLACES = [(dx, dz) for dx in range(SIDE) for dz in range(SIDE)]
NEAR = sorted(PLACES[1:], key=lambda o: min(o[0], SIDE - o[0]) + min(o[1], SIDE - o[1]))


def kernel(
    counts_hbm,
    waves_hbm,
    coupling_hbm,
    coeffs_ref,
    proj_ref,
    out_ref,
    energy_ref,
    total_ref,
    beta,
    turned,
    moved,
    lhs,
    part,
    parts_in,
    line,
    line_in,
    mixed_in,
    prod,
    weights,
    mask,
    own_energy,
    energy_in,
    group_energy,
    band_in,
    counts_ref,
    waves_ref,
    coupling_ref,
    small_sems,
    beta_sem,
    own_sem,
    in_sems,
    part_sems,
    line_sems,
    mixed_sems,
    row_sems,
    out_sems,
    energy_sems,
    band_sems,
):
    n_ga = len(PLACES)
    n_band = lax.axis_size("band")
    half = part.shape[4]
    lanes = part.shape[5]
    own = 2 * half
    slots = moved.shape[3]
    rows = beta.shape[0]
    tile = 256
    ga = lax.axis_index("ga")
    band = lax.axis_index("band")
    gx, gz = ga // SIDE, ga % SIDE

    def ahead(dx, dz):
        return lax.rem(gx + dx, SIDE) * SIDE + lax.rem(gz + dz, SIDE)

    def behind(dx, dz):
        return lax.rem(gx + SIDE - dx, SIDE) * SIDE + lax.rem(gz + SIDE - dz, SIDE)

    def columns(index):
        return pl.ds(pl.multiple_of(index * slots, 128), slots)

    def send(src, dst, sems, at, target):
        return pltpu.make_async_remote_copy(
            src,
            dst,
            sems.at[(0, *at)],
            sems.at[(1, *at)],
            device_id=target,
            device_id_type=MESH,
        )

    flat_proj = proj_ref.reshape(rows, slots)
    beta_copy = pltpu.make_async_copy(flat_proj, beta, beta_sem)

    def load_beta(t, carry):
        at = pl.ds(pl.multiple_of(t * tile, tile), tile)
        pltpu.make_async_copy(flat_proj.at[at], beta.at[at], beta_sem).start()
        return carry

    lax.fori_loop(0, rows // tile, load_beta, 0)

    def bands(h, c):
        return pl.ds(c * own + h * half, half)

    def part_rows(c):
        return pl.ds(c * half, half)

    own_copies = []
    for h in range(2):
        for c in range(2):
            own_copies.append(
                pltpu.make_async_copy(
                    coeffs_ref.at[bands(h, c), columns(ga)],
                    moved.at[h, 0, part_rows(c)],
                    own_sem.at[h, c],
                )
            )
            own_copies[-1].start()

    small_copies = [
        pltpu.make_async_copy(counts_hbm, counts_ref, small_sems.at[0]),
        pltpu.make_async_copy(waves_hbm, waves_ref, small_sems.at[1]),
        pltpu.make_async_copy(coupling_hbm, coupling_ref, small_sems.at[2]),
    ]
    for copy in small_copies:
        copy.start()

    barrier = pltpu.get_barrier_semaphore()
    for n in range(1, n_ga):
        pl.semaphore_signal(barrier, inc=1, device_id={"ga": ahead(*PLACES[n])}, device_id_type=MESH)
    for n in range(1, n_band):
        target = {"band": lax.rem(band + n, n_band)}
        pl.semaphore_signal(barrier, inc=1, device_id=target, device_id_type=MESH)
    pl.semaphore_wait(barrier, n_ga + n_band - 2)

    in_copies = [[], []]
    for h in range(2):
        for dx, dz in NEAR:
            peer, n = ahead(dx, dz), dx * SIDE + dz
            for c in range(2):
                copy = send(
                    coeffs_ref.at[bands(h, c), columns(peer)],
                    moved.at[h, n, part_rows(c)],
                    in_sems,
                    (h, n, c),
                    {"ga": peer},
                )
                copy.start()
                in_copies[h].append(copy)

    for copy in small_copies:
        copy.wait()
    slot_ids = lax.broadcasted_iota(jnp.int32, mask.shape, 1)
    mask[...] = jnp.where(slot_ids < waves_ref[0], 1.0, 0.0)
    atoms = counts_ref.shape[1]
    counts = jnp.broadcast_to(counts_ref[...].astype(jnp.float32), (atoms, atoms))
    lane_ids = lax.broadcasted_iota(jnp.int32, (atoms, atoms), 1)
    row_ids = lax.broadcasted_iota(jnp.int32, (atoms, atoms), 0)
    starts = jnp.sum(jnp.where(lane_ids < row_ids, counts, 0.0), axis=1, keepdims=True)
    lengths = jnp.sum(jnp.where(lane_ids == row_ids, counts, 0.0), axis=1, keepdims=True)
    most = coupling_ref.shape[0]
    narrow = tile // 2
    spread = jnp.where(
        lax.broadcasted_iota(jnp.int32, (narrow, tile), 1) // 2
        == lax.broadcasted_iota(jnp.int32, (narrow, tile), 0),
        1.0,
        0.0,
    )

    def weights_of(t, carry):
        at = pl.ds(pl.multiple_of(t * tile, tile), tile)
        halved = coupling_ref[:, pl.ds(pl.multiple_of(t * narrow, narrow), narrow)]
        pairs = jnp.dot(
            halved, spread, precision=lax.Precision.HIGHEST, preferred_element_type=jnp.float32
        )
        ids = t * narrow + lax.broadcasted_iota(jnp.int32, (atoms, tile), 1) // 2
        ids = ids.astype(jnp.float32)
        inside = (starts <= ids) & (ids < starts + lengths)
        first = jnp.sum(jnp.where(inside, starts, 0.0), axis=0, keepdims=True)
        length = jnp.sum(jnp.where(inside, lengths, 0.0), axis=0, keepdims=True)
        shape = (weights.shape[0], tile)
        shift = lax.broadcasted_iota(jnp.int32, shape, 0).astype(jnp.float32) - REACH
        place = shift + (ids[0:1] - first)
        sums = jnp.zeros(shape, jnp.float32)
        for k in range(most):
            row = jnp.where(k < length, pairs[k : k + 1], 0.0)
            sums = sums + jnp.where(place == k, row, 0.0)
        weights[:, at] = sums
        return carry

    lax.fori_loop(0, rows // tile, weights_of, 0)

    def even_lanes(shape):
        return lax.broadcasted_iota(jnp.int32, shape, len(shape) - 1) % 2 == 0

    def swapped(values, even):
        last = values.shape[-1]
        dim = len(values.shape) - 1
        return jnp.where(even, pltpu.roll(values, last - 1, dim), pltpu.roll(values, 1, dim))

    def place(side, first, second):
        return (first, second) if side == 0 else (second, first)

    def take_half(h):
        for copy in own_copies[2 * h : 2 * h + 2]:
            copy.wait()
        for copy in in_copies[h]:
            copy.wait_recv()
        seen = mask[0:1, :].astype(jnp.bfloat16)
        lhs[...] = moved[h].reshape(lhs.shape) * seen

    def project_side(h, side):
        sums = jnp.dot(
            lhs[...],
            turned[:, side * lanes : (side + 1) * lanes],
            preferred_element_type=jnp.float32,
        ).reshape(n_ga, 2, half, lanes)
        even = even_lanes((half, lanes))
        for first in range(SIDE):
            for second in range(SIDE):
                dx, dz = place(side, first, second)
                real, imag = sums[dx * SIDE + dz, 0], sums[dx * SIDE + dz, 1]
                pairs = jnp.where(even, real, -real) + swapped(imag, even)
                part[h, side, first, second] = pairs.astype(jnp.bfloat16)
        copies = [None]
        for k in range(1, SIDE):
            copies.append(
                send(
                    part.at[h, side, k],
                    parts_in.at[h, side, k],
                    part_sems,
                    (h, side, k),
                    {"ga": behind(*place(side, k, 0))},
                )
            )
            copies[k].start()
        return copies

    def sum_line(h, side, part_copies):
        summed = part[h, side, 0].astype(jnp.float32)
        for k in range(1, SIDE):
            part_copies[k].wait_recv()
            summed = summed + parts_in[h, side, k].astype(jnp.float32)
        line[h, side] = summed.astype(jnp.bfloat16)
        copies = [None]
        for k in range(1, SIDE):
            copies.append(
                send(
                    line.at[h, side, k],
                    line_in.at[h, side, k],
                    line_sems,
                    (h, side, k),
                    {"ga": behind(*place(side, 0, k))},
                )
            )
            copies[k].start()
        return copies

    def couple_half(h, line_copies):
        sides = []
        for side in range(2):
            summed = line[h, side, 0].astype(jnp.float32)
            for k in range(1, SIDE):
                line_copies[side][k].wait_recv()
                summed = summed + line_in[h, side, k].astype(jnp.float32)
            sides.append(summed)
        summed = jnp.concatenate(sides, axis=1)
        coupled = jnp.zeros_like(summed)
        for d in range(-REACH, REACH + 1):
            moved_by = pltpu.roll(summed, (-2 * d) % rows, 1) if d else summed
            coupled = coupled + weights[d + REACH : d + REACH + 1, :] * moved_by
        low = coupled.astype(jnp.bfloat16)
        copies = []
        for side in range(2):
            mixed_in[h, side, 0, 0] = low[:, side * lanes : (side + 1) * lanes]
            copies.append([None])
            for k in range(1, SIDE):
                copies[side].append(
                    send(
                        mixed_in.at[h, side, 0, 0],
                        mixed_in.at[h, side, 0, k],
                        mixed_sems,
                        (h, side, k),
                        {"ga": ahead(*place(side, k, 0))},
                    )
                )
                copies[side][k].start()
        terms = jnp.sum(summed * coupled, axis=1, keepdims=True) / (rows // 2)
        diagonal = lax.broadcasted_iota(
            jnp.int32, (half, 128), 0
        ) + h * half == lax.broadcasted_iota(jnp.int32, (half, 128), 1)
        return copies, jnp.sum(jnp.where(diagonal, terms, 0.0), axis=0, keepdims=True)

    def pass_on(h, mixed_copies):
        copies = []
        for side in range(2):
            for k in range(1, SIDE):
                mixed_copies[side][k].wait_recv()
            for k in range(1, SIDE):
                copies.append(
                    send(
                        mixed_in.at[h, side, 0],
                        mixed_in.at[h, side, k],
                        row_sems,
                        (h, side, k),
                        {"ga": ahead(*place(side, 0, k))},
                    )
                )
                copies[-1].start()
        return copies

    def operand_half(h, row_copies):
        for copy in row_copies:
            copy.wait_recv()

        def operand(n, carry):
            dx, dz = n // SIDE, lax.rem(n, SIDE)
            values = jnp.concatenate(
                [mixed_in[h, 0, dz, dx], mixed_in[h, 1, dx, dz]], axis=1
            ).astype(jnp.float32)
            even = even_lanes(values.shape)
            both = jnp.concatenate(
                [jnp.where(even, values, -values), swapped(values, even)], axis=0
            )
            lhs[pl.ds(pl.multiple_of(n * own, own), own), :] = both.astype(jnp.bfloat16)
            return carry

        lax.fori_loop(0, n_ga, operand, 0)

    def apply_part(h, q):
        cut = slots // 2
        at = pl.ds(q * cut, cut)
        sums = jnp.dot(lhs[...], beta[:, at], preferred_element_type=jnp.float32)
        sums = sums * mask[0:1, at]
        prod[h, :, :, at] = sums.astype(jnp.bfloat16).reshape(n_ga, own, cut)

    def to_owner(src, dst, target):
        return pltpu.make_async_remote_copy(
            src,
            dst,
            out_sems.at[0],
            out_sems.at[1],
            device_id={"ga": target},
            device_id_type=MESH,
        )

    def return_part(h, q):
        cut = slots // 2
        here = pl.ds(q * cut, cut)
        there = pl.ds(pl.multiple_of(ga * slots + q * cut, 128), cut)
        kept = []
        for dx, dz in NEAR:
            n = dx * SIDE + dz
            for c in range(2):
                to_owner(
                    prod.at[h, n, part_rows(c), here],
                    out_ref.at[bands(h, c), there],
                    behind(dx, dz),
                ).start()
        for c in range(2):
            kept.append(
                pltpu.make_async_copy(
                    prod.at[h, 0, part_rows(c), here],
                    out_ref.at[bands(h, c), there],
                    own_sem.at[2 + 2 * h + q, c],
                )
            )
            kept[-1].start()
        return kept

    beta_copy.wait()
    unit = jnp.where(
        lax.broadcasted_iota(jnp.int32, (tile, tile), 0)
        == lax.broadcasted_iota(jnp.int32, (tile, tile), 1),
        1.0,
        0.0,
    ).astype(jnp.bfloat16)
    tiles = slots // tile

    def turn(t, carry):
        here = pl.ds(pl.multiple_of(t * tile, tile), tile)
        for u in range(tiles):
            there = pl.ds(u * tile, tile)
            turned[there, here] = lax.dot_general(
                unit,
                beta[here, there],
                (((1,), (1,)), ((), ())),
                preferred_element_type=jnp.float32,
            ).astype(jnp.bfloat16)
        return carry

    lax.fori_loop(0, rows // tile, turn, 0)
    take_half(0)
    parts0 = [project_side(0, 0), project_side(0, 1)]
    take_half(1)
    parts1 = [project_side(1, 0)]
    lines0 = [sum_line(0, 0, parts0[0]), sum_line(0, 1, parts0[1])]
    parts1.append(project_side(1, 1))
    mixed0, first_terms = couple_half(0, lines0)
    lines1 = [sum_line(1, 0, parts1[0]), sum_line(1, 1, parts1[1])]
    rows0 = pass_on(0, mixed0)
    mixed1, second_terms = couple_half(1, lines1)
    terms = first_terms + second_terms
    energy_ref[...] = terms[0, :own]
    own_energy[...] = jnp.broadcast_to(jnp.sum(terms, axis=1, keepdims=True), own_energy.shape)
    energy_copies = []
    for n in range(1, n_ga):
        energy_copies.append(
            send(own_energy, energy_in.at[ga], energy_sems, (n,), {"ga": ahead(*PLACES[n])})
        )
        energy_copies[-1].start()
    operand_half(0, rows0)
    apply_part(0, 0)
    rows1 = pass_on(1, mixed1)
    returned = [return_part(0, 0)]
    apply_part(0, 1)
    returned.append(return_part(0, 1))
    operand_half(1, rows1)
    apply_part(1, 0)
    returned.append(return_part(1, 0))
    apply_part(1, 1)
    returned.append(return_part(1, 1))

    for copy in energy_copies:
        copy.wait_recv()
    energy_in[pl.ds(ga, 1)] = own_energy[...][None]
    sums = energy_in[0]
    for n in range(1, n_ga):
        sums = sums + energy_in[n]
    group_energy[...] = sums
    band_copies = []
    for n in range(1, n_band):
        target = {"band": lax.rem(band + n, n_band)}
        band_copies.append(send(group_energy, band_in.at[band], band_sems, (n,), target))
        band_copies[-1].start()
    for copy in band_copies:
        copy.wait_recv()
    band_in[pl.ds(band, 1)] = sums[None]
    sums = band_in[0]
    for n in range(1, n_band):
        sums = sums + band_in[n]
    total_ref[...] = sums[0:1, 0:1] / math.sqrt(own * n_ga * n_band)

    sent = rows0 + rows1
    for copies in parts0 + parts1 + lines0 + lines1 + mixed0 + mixed1:
        sent = sent + copies[1:]
    for copy in in_copies[0] + in_copies[1] + sent + energy_copies + band_copies:
        copy.wait_send()
    for kept in returned:
        for copy in kept:
            copy.wait()
    everything = prod.at[:, pl.ds(1, n_ga - 1)]
    whole = to_owner(everything, everything, behind(0, 1))
    whole.wait_recv()
    whole.wait_send()


def shards(coeffs, projectors, block_coupling, atom_counts, wave_counts):
    parts, own, slots_all = coeffs.shape
    rows = projectors.shape[0] * parts
    slots = projectors.shape[2]
    n_ga = lax.axis_size("ga")
    n_band = lax.axis_size("band")
    low, full = jnp.bfloat16, jnp.float32
    vmem = pl.BlockSpec(memory_space=pltpu.VMEM)
    anywhere = pl.BlockSpec(memory_space=pl.ANY)
    applied, energy, total = pl.pallas_call(
        kernel,
        out_shape=[
            jax.ShapeDtypeStruct((parts * own, slots_all), low),
            jax.ShapeDtypeStruct((own,), full),
            jax.ShapeDtypeStruct((1, 1), full),
        ],
        in_specs=[anywhere] * 5,
        out_specs=[anywhere, vmem, vmem],
        scratch_shapes=[
            pltpu.VMEM((rows, slots), low),
            pltpu.VMEM((slots, rows), low),
            pltpu.VMEM((2, n_ga, own, slots), low),
            pltpu.VMEM((n_ga * own, slots), low),
            pltpu.VMEM((2, 2, SIDE, SIDE, own // 2, rows // 2), low),
            pltpu.VMEM((2, 2, SIDE, SIDE, own // 2, rows // 2), low),
            pltpu.VMEM((2, 2, SIDE, own // 2, rows // 2), low),
            pltpu.VMEM((2, 2, SIDE, own // 2, rows // 2), low),
            pltpu.VMEM((2, 2, SIDE, SIDE, own // 2, rows // 2), low),
            pltpu.VMEM((2, n_ga, own, slots), low),
            pltpu.VMEM((40, rows), full),
            pltpu.VMEM((8, slots), full),
            pltpu.VMEM((8, 128), full),
            pltpu.VMEM((n_ga, 8, 128), full),
            pltpu.VMEM((8, 128), full),
            pltpu.VMEM((n_band, 8, 128), full),
            pltpu.VMEM((1, atom_counts.shape[0]), jnp.int32),
            pltpu.SMEM((1,), jnp.int32),
            pltpu.VMEM(block_coupling.shape[::-1], full),
            pltpu.SemaphoreType.DMA((3,)),
            pltpu.SemaphoreType.DMA,
            pltpu.SemaphoreType.DMA((6, 2)),
            pltpu.SemaphoreType.DMA((2, 2, n_ga, 2)),
            pltpu.SemaphoreType.DMA((2, 2, 2, SIDE)),
            pltpu.SemaphoreType.DMA((2, 2, 2, SIDE)),
            pltpu.SemaphoreType.DMA((2, 2, 2, SIDE)),
            pltpu.SemaphoreType.DMA((2, 2, 2, SIDE)),
            pltpu.SemaphoreType.DMA((2,)),
            pltpu.SemaphoreType.DMA((2, n_ga)),
            pltpu.SemaphoreType.DMA((2, n_band)),
        ],
        compiler_params=pltpu.CompilerParams(
            collective_id=0, has_side_effects=True, vmem_limit_bytes=56 << 20
        ),
    )(
        atom_counts.reshape(1, -1),
        wave_counts,
        block_coupling.T,
        coeffs.reshape(parts * own, slots_all),
        projectors,
    )
    return applied.reshape(coeffs.shape), energy, total[0, 0]


def solution(mesh):
    return jax.shard_map(
        shards,
        mesh=mesh,
        in_specs=(P(None, ("ga", "band"), None), P(None, None, "ga"), P(), P(), P("ga")),
        out_specs=(P(None, ("ga", "band"), None), P(("ga", "band")), P()),
        check_vma=False,
    )
```

```python
import math

import jax
import jax.numpy as jnp
from jax import lax
from jax.experimental import pallas as pl
from jax.experimental.pallas import tpu as pltpu
from jax.sharding import PartitionSpec as P

MESH = pl.DeviceIdType.MESH
SIDE = 4
REACH = 17

PLACES = [(dx, dz) for dx in range(SIDE) for dz in range(SIDE)]
NEAR = sorted(PLACES[1:], key=lambda o: min(o[0], SIDE - o[0]) + min(o[1], SIDE - o[1]))


def kernel(
    counts_hbm,
    waves_hbm,
    coupling_hbm,
    coeffs_ref,
    proj_ref,
    out_ref,
    energy_ref,
    total_ref,
    beta,
    turned,
    moved,
    lhs,
    part,
    parts_in,
    line,
    line_in,
    mixed_in,
    prod,
    weights,
    mask,
    own_energy,
    energy_in,
    group_energy,
    band_in,
    counts_ref,
    waves_ref,
    coupling_ref,
    small_sems,
    beta_sem,
    own_sem,
    in_sems,
    part_sems,
    line_sems,
    mixed_sems,
    row_sems,
    out_sems,
    energy_sems,
    band_sems,
):
    n_ga = len(PLACES)
    n_band = lax.axis_size("band")
    half = part.shape[4]
    lanes = part.shape[5]
    own = 2 * half
    slots = moved.shape[3]
    rows = beta.shape[0]
    tile = 256
    ga = lax.axis_index("ga")
    band = lax.axis_index("band")
    gx, gz = ga // SIDE, ga % SIDE

    def ahead(dx, dz):
        return lax.rem(gx + dx, SIDE) * SIDE + lax.rem(gz + dz, SIDE)

    def behind(dx, dz):
        return lax.rem(gx + SIDE - dx, SIDE) * SIDE + lax.rem(gz + SIDE - dz, SIDE)

    def columns(index):
        return pl.ds(pl.multiple_of(index * slots, 128), slots)

    def send(src, dst, sems, at, target):
        return pltpu.make_async_remote_copy(
            src,
            dst,
            sems.at[(0, *at)],
            sems.at[(1, *at)],
            device_id=target,
            device_id_type=MESH,
        )

    flat_proj = proj_ref.reshape(rows, slots)
    beta_copy = pltpu.make_async_copy(flat_proj, beta, beta_sem)

    def load_beta(t, carry):
        at = pl.ds(pl.multiple_of(t * tile, tile), tile)
        pltpu.make_async_copy(flat_proj.at[at], beta.at[at], beta_sem).start()
        return carry

    lax.fori_loop(0, rows // tile, load_beta, 0)

    def bands(h, c):
        return pl.ds(c * own + h * half, half)

    def part_rows(c):
        return pl.ds(c * half, half)

    own_copies = []
    for h in range(2):
        for c in range(2):
            own_copies.append(
                pltpu.make_async_copy(
                    coeffs_ref.at[bands(h, c), columns(ga)],
                    moved.at[h, 0, part_rows(c)],
                    own_sem.at[h, c],
                )
            )
            own_copies[-1].start()

    small_copies = [
        pltpu.make_async_copy(counts_hbm, counts_ref, small_sems.at[0]),
        pltpu.make_async_copy(waves_hbm, waves_ref, small_sems.at[1]),
        pltpu.make_async_copy(coupling_hbm, coupling_ref, small_sems.at[2]),
    ]
    for copy in small_copies:
        copy.start()

    barrier = pltpu.get_barrier_semaphore()
    for n in range(1, n_ga):
        pl.semaphore_signal(barrier, inc=1, device_id={"ga": ahead(*PLACES[n])}, device_id_type=MESH)
    for n in range(1, n_band):
        target = {"band": lax.rem(band + n, n_band)}
        pl.semaphore_signal(barrier, inc=1, device_id=target, device_id_type=MESH)
    pl.semaphore_wait(barrier, n_ga + n_band - 2)

    in_copies = [[], []]
    for h in range(2):
        for dx, dz in NEAR:
            peer, n = ahead(dx, dz), dx * SIDE + dz
            for c in range(2):
                copy = send(
                    coeffs_ref.at[bands(h, c), columns(peer)],
                    moved.at[h, n, part_rows(c)],
                    in_sems,
                    (h, n, c),
                    {"ga": peer},
                )
                copy.start()
                in_copies[h].append(copy)

    for copy in small_copies:
        copy.wait()
    slot_ids = lax.broadcasted_iota(jnp.int32, mask.shape, 1)
    mask[...] = jnp.where(slot_ids < waves_ref[0], 1.0, 0.0)
    atoms = counts_ref.shape[1]
    counts = jnp.broadcast_to(counts_ref[...].astype(jnp.float32), (atoms, atoms))
    lane_ids = lax.broadcasted_iota(jnp.int32, (atoms, atoms), 1)
    row_ids = lax.broadcasted_iota(jnp.int32, (atoms, atoms), 0)
    starts = jnp.sum(jnp.where(lane_ids < row_ids, counts, 0.0), axis=1, keepdims=True)
    lengths = jnp.sum(jnp.where(lane_ids == row_ids, counts, 0.0), axis=1, keepdims=True)
    most = coupling_ref.shape[0]
    narrow = tile // 2
    spread = jnp.where(
        lax.broadcasted_iota(jnp.int32, (narrow, tile), 1) // 2
        == lax.broadcasted_iota(jnp.int32, (narrow, tile), 0),
        1.0,
        0.0,
    )

    def weights_of(t, carry):
        at = pl.ds(pl.multiple_of(t * tile, tile), tile)
        halved = coupling_ref[:, pl.ds(pl.multiple_of(t * narrow, narrow), narrow)]
        pairs = jnp.dot(
            halved, spread, precision=lax.Precision.HIGHEST, preferred_element_type=jnp.float32
        )
        ids = t * narrow + lax.broadcasted_iota(jnp.int32, (atoms, tile), 1) // 2
        ids = ids.astype(jnp.float32)
        inside = (starts <= ids) & (ids < starts + lengths)
        first = jnp.sum(jnp.where(inside, starts, 0.0), axis=0, keepdims=True)
        length = jnp.sum(jnp.where(inside, lengths, 0.0), axis=0, keepdims=True)
        shape = (weights.shape[0], tile)
        shift = lax.broadcasted_iota(jnp.int32, shape, 0).astype(jnp.float32) - REACH
        place = shift + (ids[0:1] - first)
        sums = jnp.zeros(shape, jnp.float32)
        for k in range(most):
            row = jnp.where(k < length, pairs[k : k + 1], 0.0)
            sums = sums + jnp.where(place == k, row, 0.0)
        weights[:, at] = sums
        return carry

    lax.fori_loop(0, rows // tile, weights_of, 0)

    def even_lanes(shape):
        return lax.broadcasted_iota(jnp.int32, shape, len(shape) - 1) % 2 == 0

    def swapped(values, even):
        last = values.shape[-1]
        dim = len(values.shape) - 1
        return jnp.where(even, pltpu.roll(values, last - 1, dim), pltpu.roll(values, 1, dim))

    def place(side, first, second):
        return (first, second) if side == 0 else (second, first)

    def take_half(h):
        for copy in own_copies[2 * h : 2 * h + 2]:
            copy.wait()
        for copy in in_copies[h]:
            copy.wait_recv()
        seen = mask[0:1, :].astype(jnp.bfloat16)
        lhs[...] = moved[h].reshape(lhs.shape) * seen

    def project_side(h, side):
        sums = jnp.dot(
            lhs[...],
            turned[:, side * lanes : (side + 1) * lanes],
            preferred_element_type=jnp.float32,
        ).reshape(n_ga, 2, half, lanes)
        even = even_lanes((half, lanes))
        for first in range(SIDE):
            for second in range(SIDE):
                dx, dz = place(side, first, second)
                real, imag = sums[dx * SIDE + dz, 0], sums[dx * SIDE + dz, 1]
                pairs = jnp.where(even, real, -real) + swapped(imag, even)
                part[h, side, first, second] = pairs.astype(jnp.bfloat16)
        copies = [None]
        for k in range(1, SIDE):
            copies.append(
                send(
                    part.at[h, side, k],
                    parts_in.at[h, side, k],
                    part_sems,
                    (h, side, k),
                    {"ga": behind(*place(side, k, 0))},
                )
            )
            copies[k].start()
        return copies

    def sum_line(h, side, part_copies):
        summed = part[h, side, 0].astype(jnp.float32)
        for k in range(1, SIDE):
            part_copies[k].wait_recv()
            summed = summed + parts_in[h, side, k].astype(jnp.float32)
        line[h, side] = summed.astype(jnp.bfloat16)
        copies = [None]
        for k in range(1, SIDE):
            copies.append(
                send(
                    line.at[h, side, k],
                    line_in.at[h, side, k],
                    line_sems,
                    (h, side, k),
                    {"ga": behind(*place(side, 0, k))},
                )
            )
            copies[k].start()
        return copies

    def couple_half(h, line_copies):
        sides = []
        for side in range(2):
            summed = line[h, side, 0].astype(jnp.float32)
            for k in range(1, SIDE):
                line_copies[side][k].wait_recv()
                summed = summed + line_in[h, side, k].astype(jnp.float32)
            sides.append(summed)
        summed = jnp.concatenate(sides, axis=1)
        coupled = jnp.zeros_like(summed)
        for d in range(-REACH, REACH + 1):
            moved_by = pltpu.roll(summed, (-2 * d) % rows, 1) if d else summed
            coupled = coupled + weights[d + REACH : d + REACH + 1, :] * moved_by
        low = coupled.astype(jnp.bfloat16)
        copies = []
        for side in range(2):
            mixed_in[h, side, 0, 0] = low[:, side * lanes : (side + 1) * lanes]
            copies.append([None])
            for k in range(1, SIDE):
                copies[side].append(
                    send(
                        mixed_in.at[h, side, 0, 0],
                        mixed_in.at[h, side, 0, k],
                        mixed_sems,
                        (h, side, k),
                        {"ga": ahead(*place(side, k, 0))},
                    )
                )
                copies[side][k].start()
        terms = jnp.sum(summed * coupled, axis=1, keepdims=True) / (rows // 2)
        diagonal = lax.broadcasted_iota(
            jnp.int32, (half, 128), 0
        ) + h * half == lax.broadcasted_iota(jnp.int32, (half, 128), 1)
        return copies, jnp.sum(jnp.where(diagonal, terms, 0.0), axis=0, keepdims=True)

    def pass_on(h, mixed_copies):
        copies = []
        for side in range(2):
            for k in range(1, SIDE):
                mixed_copies[side][k].wait_recv()
            for k in range(1, SIDE):
                copies.append(
                    send(
                        mixed_in.at[h, side, 0],
                        mixed_in.at[h, side, k],
                        row_sems,
                        (h, side, k),
                        {"ga": ahead(*place(side, 0, k))},
                    )
                )
                copies[-1].start()
        return copies

    def operand_half(h, row_copies):
        for copy in row_copies:
            copy.wait_recv()

        def operand(n, carry):
            dx, dz = n // SIDE, lax.rem(n, SIDE)
            values = jnp.concatenate(
                [mixed_in[h, 0, dz, dx], mixed_in[h, 1, dx, dz]], axis=1
            ).astype(jnp.float32)
            even = even_lanes(values.shape)
            both = jnp.concatenate(
                [jnp.where(even, values, -values), swapped(values, even)], axis=0
            )
            lhs[pl.ds(pl.multiple_of(n * own, own), own), :] = both.astype(jnp.bfloat16)
            return carry

        lax.fori_loop(0, n_ga, operand, 0)

    def apply_part(h, q):
        cut = slots // 2
        at = pl.ds(q * cut, cut)
        sums = jnp.dot(lhs[...], beta[:, at], preferred_element_type=jnp.float32)
        sums = sums * mask[0:1, at]
        prod[h, :, :, at] = sums.astype(jnp.bfloat16).reshape(n_ga, own, cut)

    def to_owner(src, dst, target):
        return pltpu.make_async_remote_copy(
            src,
            dst,
            out_sems.at[0],
            out_sems.at[1],
            device_id={"ga": target},
            device_id_type=MESH,
        )

    def return_part(h, q):
        cut = slots // 2
        here = pl.ds(q * cut, cut)
        there = pl.ds(pl.multiple_of(ga * slots + q * cut, 128), cut)
        kept = []
        for dx, dz in NEAR:
            n = dx * SIDE + dz
            for c in range(2):
                to_owner(
                    prod.at[h, n, part_rows(c), here],
                    out_ref.at[bands(h, c), there],
                    behind(dx, dz),
                ).start()
        for c in range(2):
            kept.append(
                pltpu.make_async_copy(
                    prod.at[h, 0, part_rows(c), here],
                    out_ref.at[bands(h, c), there],
                    own_sem.at[2 + 2 * h + q, c],
                )
            )
            kept[-1].start()
        return kept

    beta_copy.wait()
    unit = jnp.where(
        lax.broadcasted_iota(jnp.int32, (tile, tile), 0)
        == lax.broadcasted_iota(jnp.int32, (tile, tile), 1),
        1.0,
        0.0,
    ).astype(jnp.bfloat16)
    tiles = slots // tile

    def turn(t, carry):
        here = pl.ds(pl.multiple_of(t * tile, tile), tile)
        for u in range(tiles):
            there = pl.ds(u * tile, tile)
            turned[there, here] = lax.dot_general(
                unit,
                beta[here, there],
                (((1,), (1,)), ((), ())),
                preferred_element_type=jnp.float32,
            ).astype(jnp.bfloat16)
        return carry

    lax.fori_loop(0, rows // tile, turn, 0)
    take_half(0)
    parts0 = [project_side(0, 0), project_side(0, 1)]
    take_half(1)
    parts1 = [project_side(1, 0)]
    lines0 = [sum_line(0, 0, parts0[0]), sum_line(0, 1, parts0[1])]
    parts1.append(project_side(1, 1))
    mixed0, first_terms = couple_half(0, lines0)
    lines1 = [sum_line(1, 0, parts1[0]), sum_line(1, 1, parts1[1])]
    rows0 = pass_on(0, mixed0)
    mixed1, second_terms = couple_half(1, lines1)
    terms = first_terms + second_terms
    energy_ref[...] = terms[0, :own]
    own_energy[...] = jnp.broadcast_to(jnp.sum(terms, axis=1, keepdims=True), own_energy.shape)
    energy_copies = []
    for n in range(1, n_ga):
        energy_copies.append(
            send(own_energy, energy_in.at[ga], energy_sems, (n,), {"ga": ahead(*PLACES[n])})
        )
        energy_copies[-1].start()
    operand_half(0, rows0)
    apply_part(0, 0)
    rows1 = pass_on(1, mixed1)
    returned = [return_part(0, 0)]
    apply_part(0, 1)
    returned.append(return_part(0, 1))
    operand_half(1, rows1)
    apply_part(1, 0)
    returned.append(return_part(1, 0))
    apply_part(1, 1)
    returned.append(return_part(1, 1))

    for copy in energy_copies:
        copy.wait_recv()
    energy_in[pl.ds(ga, 1)] = own_energy[...][None]
    sums = energy_in[0]
    for n in range(1, n_ga):
        sums = sums + energy_in[n]
    group_energy[...] = sums
    band_copies = []
    for n in range(1, n_band):
        target = {"band": lax.rem(band + n, n_band)}
        band_copies.append(send(group_energy, band_in.at[band], band_sems, (n,), target))
        band_copies[-1].start()
    for copy in band_copies:
        copy.wait_recv()
    band_in[pl.ds(band, 1)] = sums[None]
    sums = band_in[0]
    for n in range(1, n_band):
        sums = sums + band_in[n]
    total_ref[...] = sums[0:1, 0:1] / math.sqrt(own * n_ga * n_band)

    sent = rows0 + rows1
    for copies in parts0 + parts1 + lines0 + lines1 + mixed0 + mixed1:
        sent = sent + copies[1:]
    for copy in in_copies[0] + in_copies[1] + sent + energy_copies + band_copies:
        copy.wait_send()
    for kept in returned:
        for copy in kept:
            copy.wait()
    everything = prod.at[:, pl.ds(1, n_ga - 1)]
    whole = to_owner(everything, everything, behind(0, 1))
    whole.wait_recv()
    whole.wait_send()


def deliver(applied_ref, energy_ref, total_ref, applied_out, energy_out, total_out, row, one, sems):
    pieces = sems.shape[0] - 4
    cut = applied_ref.shape[1] // pieces
    copies = []
    for k in range(pieces):
        at = pl.ds(k * cut, cut)
        copies.append(pltpu.make_async_copy(applied_ref.at[:, at], applied_out.at[:, at], sems.at[k]))
        copies[k].start()
    small = ((energy_ref, row, energy_out, pieces), (total_ref, one, total_out, pieces + 2))
    ins = [pltpu.make_async_copy(ref, kept, sems.at[k]) for ref, kept, _, k in small]
    outs = [pltpu.make_async_copy(kept, out, sems.at[k + 1]) for _, kept, out, k in small]
    for copy in ins:
        copy.start()
    for before, after in zip(ins, outs):
        before.wait()
        after.start()
    for copy in copies + outs:
        copy.wait()


def shards(coeffs, projectors, block_coupling, atom_counts, wave_counts):
    parts, own, slots_all = coeffs.shape
    rows = projectors.shape[0] * parts
    slots = projectors.shape[2]
    n_ga = lax.axis_size("ga")
    n_band = lax.axis_size("band")
    low, full = jnp.bfloat16, jnp.float32
    vmem = pl.BlockSpec(memory_space=pltpu.VMEM)
    anywhere = pl.BlockSpec(memory_space=pl.ANY)
    applied, energy, total = pl.pallas_call(
        kernel,
        out_shape=[
            pltpu.VMEM((parts * own, slots_all), low),
            jax.ShapeDtypeStruct((own,), full),
            jax.ShapeDtypeStruct((1, 1), full),
        ],
        in_specs=[anywhere] * 5,
        out_specs=[vmem, vmem, vmem],
        scratch_shapes=[
            pltpu.VMEM((rows, slots), low),
            pltpu.VMEM((slots, rows), low),
            pltpu.VMEM((2, n_ga, own, slots), low),
            pltpu.VMEM((n_ga * own, slots), low),
            pltpu.VMEM((2, 2, SIDE, SIDE, own // 2, rows // 2), low),
            pltpu.VMEM((2, 2, SIDE, SIDE, own // 2, rows // 2), low),
            pltpu.VMEM((2, 2, SIDE, own // 2, rows // 2), low),
            pltpu.VMEM((2, 2, SIDE, own // 2, rows // 2), low),
            pltpu.VMEM((2, 2, SIDE, SIDE, own // 2, rows // 2), low),
            pltpu.VMEM((2, n_ga, own, slots), low),
            pltpu.VMEM((40, rows), full),
            pltpu.VMEM((8, slots), full),
            pltpu.VMEM((8, 128), full),
            pltpu.VMEM((n_ga, 8, 128), full),
            pltpu.VMEM((8, 128), full),
            pltpu.VMEM((n_band, 8, 128), full),
            pltpu.VMEM((1, atom_counts.shape[0]), jnp.int32),
            pltpu.SMEM((1,), jnp.int32),
            pltpu.VMEM(block_coupling.shape[::-1], full),
            pltpu.SemaphoreType.DMA((3,)),
            pltpu.SemaphoreType.DMA,
            pltpu.SemaphoreType.DMA((6, 2)),
            pltpu.SemaphoreType.DMA((2, 2, n_ga, 2)),
            pltpu.SemaphoreType.DMA((2, 2, 2, SIDE)),
            pltpu.SemaphoreType.DMA((2, 2, 2, SIDE)),
            pltpu.SemaphoreType.DMA((2, 2, 2, SIDE)),
            pltpu.SemaphoreType.DMA((2, 2, 2, SIDE)),
            pltpu.SemaphoreType.DMA((2,)),
            pltpu.SemaphoreType.DMA((2, n_ga)),
            pltpu.SemaphoreType.DMA((2, n_band)),
        ],
        compiler_params=pltpu.CompilerParams(
            collective_id=0, has_side_effects=True, vmem_limit_bytes=56 << 20
        ),
    )(
        atom_counts.reshape(1, -1),
        wave_counts,
        block_coupling.T,
        coeffs.reshape(parts * own, slots_all),
        projectors,
    )
    shapes = [jax.ShapeDtypeStruct(x.shape, x.dtype) for x in (applied, energy, total)]
    pieces = 8
    applied, energy, total = pl.pallas_call(
        deliver,
        out_shape=shapes,
        in_specs=[vmem, anywhere, anywhere],
        out_specs=[anywhere] * 3,
        scratch_shapes=[
            pltpu.VMEM(energy.shape, full),
            pltpu.VMEM(total.shape, full),
            pltpu.SemaphoreType.DMA((pieces + 4,)),
        ],
        compiler_params=pltpu.CompilerParams(vmem_limit_bytes=56 << 20),
    )(applied, energy, total)
    return applied.reshape(coeffs.shape), energy, total[0, 0]


def solution(mesh):
    return jax.shard_map(
        shards,
        mesh=mesh,
        in_specs=(P(None, ("ga", "band"), None), P(None, None, "ga"), P(), P(), P("ga")),
        out_specs=(P(None, ("ga", "band"), None), P(("ga", "band")), P()),
        check_vma=False,
    )
```

```python
import math

import jax
import jax.numpy as jnp
from jax import lax
from jax.experimental import pallas as pl
from jax.experimental.pallas import tpu as pltpu
from jax.sharding import PartitionSpec as P

MESH = pl.DeviceIdType.MESH
SIDE = 4
REACH = 17

PLACES = [(dx, dz) for dx in range(SIDE) for dz in range(SIDE)]
NEAR = sorted(PLACES[1:], key=lambda o: min(o[0], SIDE - o[0]) + min(o[1], SIDE - o[1]))


def kernel(
    counts_hbm,
    waves_hbm,
    coupling_hbm,
    coeffs_ref,
    proj_ref,
    out_ref,
    energy_ref,
    total_ref,
    beta,
    turned,
    moved,
    lhs,
    part,
    parts_in,
    line,
    line_in,
    mixed_in,
    prod,
    weights,
    mask,
    own_energy,
    energy_in,
    group_energy,
    band_in,
    counts_ref,
    waves_ref,
    coupling_ref,
    small_sems,
    beta_sem,
    own_sem,
    in_sems,
    part_sems,
    line_sems,
    mixed_sems,
    row_sems,
    out_sems,
    energy_sems,
    band_sems,
):
    n_ga = len(PLACES)
    n_band = lax.axis_size("band")
    half = part.shape[4]
    lanes = part.shape[5]
    own = 2 * half
    slots = moved.shape[3]
    rows = beta.shape[0]
    tile = 256
    ga = lax.axis_index("ga")
    band = lax.axis_index("band")
    gx, gz = ga // SIDE, ga % SIDE

    def ahead(dx, dz):
        return lax.rem(gx + dx, SIDE) * SIDE + lax.rem(gz + dz, SIDE)

    def behind(dx, dz):
        return lax.rem(gx + SIDE - dx, SIDE) * SIDE + lax.rem(gz + SIDE - dz, SIDE)

    def columns(index):
        return pl.ds(pl.multiple_of(index * slots, 128), slots)

    def send(src, dst, sems, at, target):
        return pltpu.make_async_remote_copy(
            src,
            dst,
            sems.at[(0, *at)],
            sems.at[(1, *at)],
            device_id=target,
            device_id_type=MESH,
        )

    flat_proj = proj_ref.reshape(rows, slots)
    beta_copy = pltpu.make_async_copy(flat_proj, beta, beta_sem)

    def load_beta(t, carry):
        at = pl.ds(pl.multiple_of(t * tile, tile), tile)
        pltpu.make_async_copy(flat_proj.at[at], beta.at[at], beta_sem).start()
        return carry

    lax.fori_loop(0, rows // tile, load_beta, 0)

    def bands(h, c):
        return pl.ds(c * own + h * half, half)

    def part_rows(c):
        return pl.ds(c * half, half)

    own_copies = []
    for h in range(2):
        for c in range(2):
            own_copies.append(
                pltpu.make_async_copy(
                    coeffs_ref.at[bands(h, c), columns(ga)],
                    moved.at[h, 0, part_rows(c)],
                    own_sem.at[h, c],
                )
            )
            own_copies[-1].start()

    small_copies = [
        pltpu.make_async_copy(counts_hbm, counts_ref, small_sems.at[0]),
        pltpu.make_async_copy(waves_hbm, waves_ref, small_sems.at[1]),
        pltpu.make_async_copy(coupling_hbm, coupling_ref, small_sems.at[2]),
    ]
    for copy in small_copies:
        copy.start()

    barrier = pltpu.get_barrier_semaphore()
    for n in range(1, n_ga):
        pl.semaphore_signal(barrier, inc=1, device_id={"ga": ahead(*PLACES[n])}, device_id_type=MESH)
    for n in range(1, n_band):
        target = {"band": lax.rem(band + n, n_band)}
        pl.semaphore_signal(barrier, inc=1, device_id=target, device_id_type=MESH)
    pl.semaphore_wait(barrier, n_ga + n_band - 2)

    in_copies = [[], []]
    for h in range(2):
        for dx, dz in NEAR:
            peer, n = ahead(dx, dz), dx * SIDE + dz
            for c in range(2):
                copy = send(
                    coeffs_ref.at[bands(h, c), columns(peer)],
                    moved.at[h, n, part_rows(c)],
                    in_sems,
                    (h, n, c),
                    {"ga": peer},
                )
                copy.start()
                in_copies[h].append(copy)

    for copy in small_copies:
        copy.wait()
    slot_ids = lax.broadcasted_iota(jnp.int32, mask.shape, 1)
    mask[...] = jnp.where(slot_ids < waves_ref[0], 1.0, 0.0)
    atoms = counts_ref.shape[1]
    counts = jnp.broadcast_to(counts_ref[...].astype(jnp.float32), (atoms, atoms))
    lane_ids = lax.broadcasted_iota(jnp.int32, (atoms, atoms), 1)
    row_ids = lax.broadcasted_iota(jnp.int32, (atoms, atoms), 0)
    starts = jnp.sum(jnp.where(lane_ids < row_ids, counts, 0.0), axis=1, keepdims=True)
    lengths = jnp.sum(jnp.where(lane_ids == row_ids, counts, 0.0), axis=1, keepdims=True)
    most = coupling_ref.shape[0]
    narrow = tile // 2
    spread = jnp.where(
        lax.broadcasted_iota(jnp.int32, (narrow, tile), 1) // 2
        == lax.broadcasted_iota(jnp.int32, (narrow, tile), 0),
        1.0,
        0.0,
    )

    def weights_of(t, carry):
        at = pl.ds(pl.multiple_of(t * tile, tile), tile)
        halved = coupling_ref[:, pl.ds(pl.multiple_of(t * narrow, narrow), narrow)]
        pairs = jnp.dot(
            halved, spread, precision=lax.Precision.HIGHEST, preferred_element_type=jnp.float32
        )
        ids = t * narrow + lax.broadcasted_iota(jnp.int32, (atoms, tile), 1) // 2
        ids = ids.astype(jnp.float32)
        inside = (starts <= ids) & (ids < starts + lengths)
        first = jnp.sum(jnp.where(inside, starts, 0.0), axis=0, keepdims=True)
        length = jnp.sum(jnp.where(inside, lengths, 0.0), axis=0, keepdims=True)
        shape = (weights.shape[0], tile)
        shift = lax.broadcasted_iota(jnp.int32, shape, 0).astype(jnp.float32) - REACH
        place = shift + (ids[0:1] - first)
        sums = jnp.zeros(shape, jnp.float32)
        for k in range(most):
            row = jnp.where(k < length, pairs[k : k + 1], 0.0)
            sums = sums + jnp.where(place == k, row, 0.0)
        weights[:, at] = sums
        return carry

    lax.fori_loop(0, rows // tile, weights_of, 0)

    def even_lanes(shape):
        return lax.broadcasted_iota(jnp.int32, shape, len(shape) - 1) % 2 == 0

    def swapped(values, even):
        last = values.shape[-1]
        dim = len(values.shape) - 1
        return jnp.where(even, pltpu.roll(values, last - 1, dim), pltpu.roll(values, 1, dim))

    def place(side, first, second):
        return (first, second) if side == 0 else (second, first)

    def take_half(h):
        for copy in own_copies[2 * h : 2 * h + 2]:
            copy.wait()
        for copy in in_copies[h]:
            copy.wait_recv()
        seen = mask[0:1, :].astype(jnp.bfloat16)
        lhs[...] = moved[h].reshape(lhs.shape) * seen

    def project_side(h, side):
        sums = jnp.dot(
            lhs[...],
            turned[:, side * lanes : (side + 1) * lanes],
            preferred_element_type=jnp.float32,
        ).reshape(n_ga, 2, half, lanes)
        even = even_lanes((half, lanes))
        for first in range(SIDE):
            for second in range(SIDE):
                dx, dz = place(side, first, second)
                real, imag = sums[dx * SIDE + dz, 0], sums[dx * SIDE + dz, 1]
                pairs = jnp.where(even, real, -real) + swapped(imag, even)
                part[h, side, first, second] = pairs.astype(jnp.bfloat16)
        copies = [None]
        for k in range(1, SIDE):
            copies.append(
                send(
                    part.at[h, side, k],
                    parts_in.at[h, side, k],
                    part_sems,
                    (h, side, k),
                    {"ga": behind(*place(side, k, 0))},
                )
            )
            copies[k].start()
        return copies

    def sum_line(h, side, part_copies):
        summed = part[h, side, 0].astype(jnp.float32)
        for k in range(1, SIDE):
            part_copies[k].wait_recv()
            summed = summed + parts_in[h, side, k].astype(jnp.float32)
        line[h, side] = summed.astype(jnp.bfloat16)
        copies = [None]
        for k in range(1, SIDE):
            copies.append(
                send(
                    line.at[h, side, k],
                    line_in.at[h, side, k],
                    line_sems,
                    (h, side, k),
                    {"ga": behind(*place(side, 0, k))},
                )
            )
            copies[k].start()
        return copies

    def couple_half(h, line_copies):
        sides = []
        for side in range(2):
            summed = line[h, side, 0].astype(jnp.float32)
            for k in range(1, SIDE):
                line_copies[side][k].wait_recv()
                summed = summed + line_in[h, side, k].astype(jnp.float32)
            sides.append(summed)
        summed = jnp.concatenate(sides, axis=1)
        coupled = jnp.zeros_like(summed)
        for d in range(-REACH, REACH + 1):
            moved_by = pltpu.roll(summed, (-2 * d) % rows, 1) if d else summed
            coupled = coupled + weights[d + REACH : d + REACH + 1, :] * moved_by
        low = coupled.astype(jnp.bfloat16)
        copies = []
        for side in range(2):
            mixed_in[h, side, 0, 0] = low[:, side * lanes : (side + 1) * lanes]
            copies.append([None])
            for k in range(1, SIDE):
                copies[side].append(
                    send(
                        mixed_in.at[h, side, 0, 0],
                        mixed_in.at[h, side, 0, k],
                        mixed_sems,
                        (h, side, k),
                        {"ga": ahead(*place(side, k, 0))},
                    )
                )
                copies[side][k].start()
        terms = jnp.sum(summed * coupled, axis=1, keepdims=True) / (rows // 2)
        diagonal = lax.broadcasted_iota(
            jnp.int32, (half, 128), 0
        ) + h * half == lax.broadcasted_iota(jnp.int32, (half, 128), 1)
        return copies, jnp.sum(jnp.where(diagonal, terms, 0.0), axis=0, keepdims=True)

    def pass_on(h, mixed_copies):
        copies = []
        for side in range(2):
            for k in range(1, SIDE):
                mixed_copies[side][k].wait_recv()
            for k in range(1, SIDE):
                copies.append(
                    send(
                        mixed_in.at[h, side, 0],
                        mixed_in.at[h, side, k],
                        row_sems,
                        (h, side, k),
                        {"ga": ahead(*place(side, 0, k))},
                    )
                )
                copies[-1].start()
        return copies

    def operand_half(h, row_copies):
        for copy in row_copies:
            copy.wait_recv()

        def operand(n, carry):
            dx, dz = n // SIDE, lax.rem(n, SIDE)
            values = jnp.concatenate(
                [mixed_in[h, 0, dz, dx], mixed_in[h, 1, dx, dz]], axis=1
            ).astype(jnp.float32)
            even = even_lanes(values.shape)
            both = jnp.concatenate(
                [jnp.where(even, values, -values), swapped(values, even)], axis=0
            )
            lhs[pl.ds(pl.multiple_of(n * own, own), own), :] = both.astype(jnp.bfloat16)
            return carry

        lax.fori_loop(0, n_ga, operand, 0)

    def apply_part(h, q):
        cut = slots // 2
        at = pl.ds(q * cut, cut)
        sums = jnp.dot(lhs[...], beta[:, at], preferred_element_type=jnp.float32)
        sums = sums * mask[0:1, at]
        prod[h, :, :, at] = sums.astype(jnp.bfloat16).reshape(n_ga, own, cut)

    def to_owner(src, dst, target):
        return pltpu.make_async_remote_copy(
            src,
            dst,
            out_sems.at[0],
            out_sems.at[1],
            device_id={"ga": target},
            device_id_type=MESH,
        )

    def return_part(h, q):
        cut = slots // 2
        here = pl.ds(q * cut, cut)
        there = pl.ds(pl.multiple_of(ga * slots + q * cut, 128), cut)
        kept = []
        for dx, dz in NEAR:
            n = dx * SIDE + dz
            for c in range(2):
                to_owner(
                    prod.at[h, n, part_rows(c), here],
                    out_ref.at[bands(h, c), there],
                    behind(dx, dz),
                ).start()
        for c in range(2):
            kept.append(
                pltpu.make_async_copy(
                    prod.at[h, 0, part_rows(c), here],
                    out_ref.at[bands(h, c), there],
                    own_sem.at[2 + 2 * h + q, c],
                )
            )
            kept[-1].start()
        return kept

    beta_copy.wait()
    unit = jnp.where(
        lax.broadcasted_iota(jnp.int32, (tile, tile), 0)
        == lax.broadcasted_iota(jnp.int32, (tile, tile), 1),
        1.0,
        0.0,
    ).astype(jnp.bfloat16)
    tiles = slots // tile

    def turn(t, carry):
        here = pl.ds(pl.multiple_of(t * tile, tile), tile)
        for u in range(tiles):
            there = pl.ds(u * tile, tile)
            turned[there, here] = lax.dot_general(
                unit,
                beta[here, there],
                (((1,), (1,)), ((), ())),
                preferred_element_type=jnp.float32,
            ).astype(jnp.bfloat16)
        return carry

    lax.fori_loop(0, rows // tile, turn, 0)
    take_half(0)
    parts0 = [project_side(0, 0), project_side(0, 1)]
    take_half(1)
    parts1 = [project_side(1, 0)]
    lines0 = [sum_line(0, 0, parts0[0]), sum_line(0, 1, parts0[1])]
    parts1.append(project_side(1, 1))
    mixed0, first_terms = couple_half(0, lines0)
    lines1 = [sum_line(1, 0, parts1[0]), sum_line(1, 1, parts1[1])]
    rows0 = pass_on(0, mixed0)
    mixed1, second_terms = couple_half(1, lines1)
    terms = first_terms + second_terms
    energy_ref[...] = terms[0, :own]
    own_energy[...] = jnp.broadcast_to(jnp.sum(terms, axis=1, keepdims=True), own_energy.shape)
    energy_copies = []
    for n in range(1, n_ga):
        energy_copies.append(
            send(own_energy, energy_in.at[ga], energy_sems, (n,), {"ga": ahead(*PLACES[n])})
        )
        energy_copies[-1].start()
    operand_half(0, rows0)
    apply_part(0, 0)
    rows1 = pass_on(1, mixed1)
    returned = [return_part(0, 0)]
    apply_part(0, 1)
    returned.append(return_part(0, 1))
    operand_half(1, rows1)
    apply_part(1, 0)
    returned.append(return_part(1, 0))
    apply_part(1, 1)
    returned.append(return_part(1, 1))

    for copy in energy_copies:
        copy.wait_recv()
    energy_in[pl.ds(ga, 1)] = own_energy[...][None]
    sums = energy_in[0]
    for n in range(1, n_ga):
        sums = sums + energy_in[n]
    group_energy[...] = sums
    band_copies = []
    for n in range(1, n_band):
        target = {"band": lax.rem(band + n, n_band)}
        band_copies.append(send(group_energy, band_in.at[band], band_sems, (n,), target))
        band_copies[-1].start()
    for copy in band_copies:
        copy.wait_recv()
    band_in[pl.ds(band, 1)] = sums[None]
    sums = band_in[0]
    for n in range(1, n_band):
        sums = sums + band_in[n]
    total_ref[...] = sums[0:1, 0:1] / math.sqrt(own * n_ga * n_band)

    sent = rows0 + rows1
    for copies in parts0 + parts1 + lines0 + lines1 + mixed0 + mixed1:
        sent = sent + copies[1:]
    for copy in in_copies[0] + in_copies[1] + sent + energy_copies + band_copies:
        copy.wait_send()
    for kept in returned:
        for copy in kept:
            copy.wait()
    everything = prod.at[:, pl.ds(1, n_ga - 1)]
    whole = to_owner(everything, everything, behind(0, 1))
    whole.wait_recv()
    whole.wait_send()


def deliver(applied_ref, energy_ref, total_ref, applied_out, energy_out, total_out, row, one, sems):
    pieces = sems.shape[0] - 4
    cut = applied_ref.shape[1] // pieces
    copies = []
    for k in range(pieces):
        at = pl.ds(k * cut, cut)
        copies.append(pltpu.make_async_copy(applied_ref.at[:, at], applied_out.at[:, at], sems.at[k]))
        copies[k].start()
    small = ((energy_ref, row, energy_out, pieces), (total_ref, one, total_out, pieces + 2))
    ins = [pltpu.make_async_copy(ref, kept, sems.at[k]) for ref, kept, _, k in small]
    outs = [pltpu.make_async_copy(kept, out, sems.at[k + 1]) for _, kept, out, k in small]
    for copy in ins:
        copy.start()
    for before, after in zip(ins, outs):
        before.wait()
        after.start()
    for copy in copies + outs:
        copy.wait()


def shards(coeffs, projectors, block_coupling, atom_counts, wave_counts):
    parts, own, slots_all = coeffs.shape
    rows = projectors.shape[0] * parts
    slots = projectors.shape[2]
    n_ga = lax.axis_size("ga")
    n_band = lax.axis_size("band")
    low, full = jnp.bfloat16, jnp.float32
    vmem = pl.BlockSpec(memory_space=pltpu.VMEM)
    anywhere = pl.BlockSpec(memory_space=pl.ANY)
    applied, energy, total = pl.pallas_call(
        kernel,
        out_shape=[
            pltpu.VMEM((parts * own, slots_all), low),
            jax.ShapeDtypeStruct((own,), full),
            jax.ShapeDtypeStruct((1, 1), full),
        ],
        in_specs=[anywhere] * 5,
        out_specs=[vmem, vmem, vmem],
        scratch_shapes=[
            pltpu.VMEM((rows, slots), low),
            pltpu.VMEM((slots, rows), low),
            pltpu.VMEM((2, n_ga, own, slots), low),
            pltpu.VMEM((n_ga * own, slots), low),
            pltpu.VMEM((2, 2, SIDE, SIDE, own // 2, rows // 2), low),
            pltpu.VMEM((2, 2, SIDE, SIDE, own // 2, rows // 2), low),
            pltpu.VMEM((2, 2, SIDE, own // 2, rows // 2), low),
            pltpu.VMEM((2, 2, SIDE, own // 2, rows // 2), low),
            pltpu.VMEM((2, 2, SIDE, SIDE, own // 2, rows // 2), low),
            pltpu.VMEM((2, n_ga, own, slots), low),
            pltpu.VMEM((40, rows), full),
            pltpu.VMEM((8, slots), full),
            pltpu.VMEM((8, 128), full),
            pltpu.VMEM((n_ga, 8, 128), full),
            pltpu.VMEM((8, 128), full),
            pltpu.VMEM((n_band, 8, 128), full),
            pltpu.VMEM((1, atom_counts.shape[0]), jnp.int32),
            pltpu.SMEM((1,), jnp.int32),
            pltpu.VMEM(block_coupling.shape[::-1], full),
            pltpu.SemaphoreType.DMA((3,)),
            pltpu.SemaphoreType.DMA,
            pltpu.SemaphoreType.DMA((6, 2)),
            pltpu.SemaphoreType.DMA((2, 2, n_ga, 2)),
            pltpu.SemaphoreType.DMA((2, 2, 2, SIDE)),
            pltpu.SemaphoreType.DMA((2, 2, 2, SIDE)),
            pltpu.SemaphoreType.DMA((2, 2, 2, SIDE)),
            pltpu.SemaphoreType.DMA((2, 2, 2, SIDE)),
            pltpu.SemaphoreType.DMA((2,)),
            pltpu.SemaphoreType.DMA((2, n_ga)),
            pltpu.SemaphoreType.DMA((2, n_band)),
        ],
        compiler_params=pltpu.CompilerParams(
            collective_id=0, has_side_effects=True, vmem_limit_bytes=56 << 20
        ),
    )(
        atom_counts.reshape(1, -1),
        wave_counts,
        block_coupling.T,
        coeffs.reshape(parts * own, slots_all),
        projectors,
    )
    shapes = [jax.ShapeDtypeStruct(x.shape, x.dtype) for x in (applied, energy, total)]
    pieces = 8
    applied, energy, total = pl.pallas_call(
        deliver,
        out_shape=shapes,
        in_specs=[vmem, anywhere, anywhere],
        out_specs=[anywhere] * 3,
        scratch_shapes=[
            pltpu.VMEM(energy.shape, full),
            pltpu.VMEM(total.shape, full),
            pltpu.SemaphoreType.DMA((pieces + 4,)),
        ],
        compiler_params=pltpu.CompilerParams(vmem_limit_bytes=56 << 20),
    )(pltpu.with_memory_space_constraint(applied, pltpu.VMEM), energy, total)
    return applied.reshape(coeffs.shape), energy, total[0, 0]


def solution(mesh):
    return jax.shard_map(
        shards,
        mesh=mesh,
        in_specs=(P(None, ("ga", "band"), None), P(None, None, "ga"), P(), P(), P("ga")),
        out_specs=(P(None, ("ga", "band"), None), P(("ga", "band")), P()),
        check_vma=False,
    )
```
